32 devices in a mesh: seq: 8 (over y, x, core), head: 4 (over z).
Axes of the slice: x: 2, y: 2, z: 4, core: 2. Of those that a mesh axis runs over, the one named last changes fastest.
Arguments:
- tokens: bfloat16 [32, 1024, 1024], P('seq'), may hold values from -6 to 6
- w_query: bfloat16 [1024, 1024], P(None, 'head'), may hold values from -1 to 1
- w_key: bfloat16 [1024, 1024], P(None, 'head'), may hold values from -1 to 1
- w_value: bfloat16 [1024, 1024], P(None, 'head'), may hold values from -0.1875 to 0.1875
- w_out: bfloat16 [1024, 1024], P('head'), may hold values from -0.1875 to 0.1875
Outputs:
- mixed: bfloat16 [32, 1024, 1024], P('seq', None, 'head')
The draws below stay inside these ranges and needn't reach their ends.
All inputs are finite; a program needn't handle non-finite values.
Results may differ from the reference program's by a relative error of at most 0.012.
Values may be sent and summed in bfloat16 or wider, within the bound.
No kernel may reach another device: no remote copies, remote signals or barrier semaphores. Data moves between devices by JAX's collectives and lax.ppermute only.
A program may use at most 128 MiB of HBM per device.

```python
import jax
import jax.numpy as jnp
from jax import lax

D = 1024
HEADS = 16
FRAMES = 32
PATCHES = 1024


def query_key_pair(key):
    shape_full = (D, D)
    base = jnp.clip(jax.random.normal(jax.random.fold_in(key, 11), shape_full, jnp.float32), -6.0, 6.0)
    other = jnp.clip(jax.random.normal(jax.random.fold_in(key, 12), shape_full, jnp.float32), -6.0, 6.0)
    return (base * D ** (-0.5), other * D ** (-0.5))


def draw_w_query(key, part):
    first, second = query_key_pair(key)
    return first.astype(jnp.bfloat16)


def draw_w_key(key, part):
    first, second = query_key_pair(key)
    return second.astype(jnp.bfloat16)


def steps_of(own_key, extent, shards, low, high):
    level = 1.0
    for dim, parts in shards:
        draws = jax.random.uniform(jax.random.fold_in(jax.random.fold_in(own_key, 6), dim), (parts,), jnp.float32, low / len(shards), high / len(shards))
        level = level * jnp.repeat(jnp.exp(draws), extent[dim] // parts).reshape((-1,) + (1,) * (len(extent) - 1 - dim))
    return level


def noise(rng, extent, spread, limit, split=(), dtype=jnp.bfloat16):
    array = spread * jax.random.normal(rng, extent, jnp.float32)
    if split:
        array = array * steps_of(rng, extent, split, -0.22, 0.18)
    return jnp.clip(array, -limit, limit).astype(dtype)


def setup_inputs(seed: int = 0) -> dict:
    streams_of = jax.random.split(jax.random.key(seed), 6)
    tokens = noise(streams_of[0], (FRAMES, PATCHES, D), 1.0, 6.0, ((0, 8),))
    w_query = draw_w_query(jax.random.fold_in(streams_of[5], 71), 0)
    w_key = draw_w_key(jax.random.fold_in(streams_of[5], 71), 0)
    w_value = noise(streams_of[3], (D, D), D ** -0.5, 0.1875, ((1, 4),))
    w_out = noise(streams_of[4], (D, D), D ** -0.5, 0.1875, ((0, 4),))
    return {"tokens": tokens, "w_query": w_query, "w_key": w_key, "w_value": w_value, "w_out": w_out}


epsilon = 1e-05

def normalize(tokens):
    values = tokens.astype(jnp.float32)
    row_mean = lax.optimization_barrier(jnp.mean(values, axis=-1, keepdims=True))
    centered = values - row_mean
    row_var = lax.optimization_barrier(jnp.mean(centered * centered, axis=-1, keepdims=True))
    return (centered * lax.rsqrt(row_var + epsilon)).astype(jnp.bfloat16)

def project(source, weight):
    frames, patch_count, width = source.shape
    flat = jnp.dot(source.reshape(frames * patch_count, width), weight, preferred_element_type=jnp.float32)
    return flat.astype(jnp.bfloat16).reshape(frames, patch_count, weight.shape[1])

def attend(queries, key_rows, value_rows, head_count):
    frames, patch_count, feature_width = queries.shape
    head_size = feature_width // head_count
    query_flat = queries.reshape(frames, patch_count * head_count, head_size).astype(jnp.float32)
    key_flat = key_rows.reshape(frames, patch_count * head_count, head_size).astype(jnp.float32)
    value_flat = value_rows.reshape(frames, patch_count * head_count, head_size).astype(jnp.float32)
    scores = jnp.einsum('fmd,gmd->fgm', query_flat, key_flat) * head_size ** (-0.5)
    row_top = lax.optimization_barrier(jnp.max(scores, axis=1, keepdims=True))
    raised = jnp.exp(scores - row_top)
    weights = (raised / lax.optimization_barrier(jnp.sum(raised, axis=1, keepdims=True))).astype(jnp.bfloat16)
    attended = jnp.einsum('fgm,gmd->fmd', weights.astype(jnp.float32), value_flat)
    return attended.astype(jnp.bfloat16).reshape(frames, patch_count, feature_width)

def reference(tokens, w_query, w_key, w_value, w_out):
    normed = normalize(tokens)
    queries = project(normed, w_query)
    key_rows = project(normed, w_key)
    value_rows = project(normed, w_value)
    attended = attend(queries, key_rows, value_rows, HEADS)
    return project(attended, w_out)
```

```python
import functools

import jax
import jax.numpy as jnp
from jax import lax
from jax.experimental import pallas as pl
from jax.experimental.pallas import tpu as pltpu
from jax.sharding import PartitionSpec as P

HS = 64
GROUP = 4
LANES = 128

epsilon = 1e-05


def block_kernel(x_ref, w_ref, o_ref, *, groups):
    width = x_ref.shape[-1]
    heads, seq, rows, packed = w_ref.shape
    cols = packed // 4
    splits = seq // heads
    count = x_ref.shape[0] * x_ref.shape[2]
    x = jnp.concatenate([x_ref[:, g].reshape(count, width) for g in range(groups)], axis=0)
    values = x.astype(jnp.float32)
    centered = values - jnp.mean(values, axis=-1, keepdims=True)
    row_var = jnp.mean(centered * centered, axis=-1, keepdims=True)
    normed = (centered * lax.rsqrt(row_var + epsilon)).astype(jnp.bfloat16)
    row = lax.broadcasted_iota(jnp.int32, (2 * count, count), 0)
    col = lax.broadcasted_iota(jnp.int32, (2 * count, count), 1)
    same = (row % GROUP) == (col % GROUP)
    lane = lax.broadcasted_iota(jnp.int32, (count, LANES), 1)
    first = lane < HS
    attended = []
    for h in range(heads):
        weight = w_ref[h].reshape(seq * rows, packed)[:, : 3 * cols]
        qkv = jnp.dot(normed, weight, preferred_element_type=jnp.float32).astype(jnp.bfloat16)
        for pair in range(cols // LANES):
            parts = []
            for g in range(groups):
                span = slice(g * count, (g + 1) * count)
                at = pair * LANES
                q = qkv[span, at : at + LANES] * jnp.bfloat16(HS ** (-0.5))
                k = qkv[span, cols + at : cols + at + LANES]
                v = qkv[span, 2 * cols + at : 2 * cols + at + LANES]
                zero = jnp.zeros_like(q)
                both = jnp.concatenate([jnp.where(first, q, zero), jnp.where(first, zero, q)], axis=0)
                scores = lax.dot_general(
                    both, k, (((1,), (1,)), ((), ())), preferred_element_type=jnp.float32
                )
                scores = jnp.where(same, scores, -1e30)
                raised = jnp.exp(scores - jnp.max(scores, axis=1, keepdims=True))
                weights = (raised / jnp.sum(raised, axis=1, keepdims=True)).astype(jnp.bfloat16)
                out = jnp.dot(weights, v, preferred_element_type=jnp.float32)
                parts.append(jnp.where(first, out[:count], out[count:]).astype(jnp.bfloat16))
            attended.append(jnp.concatenate(parts, axis=0))
    attended = jnp.concatenate(attended, axis=1)
    for c in range(heads):
        total = None
        for h in range(heads):
            block = w_ref[h, c * splits : (c + 1) * splits, :, 3 * cols :].reshape(splits * rows, cols)
            piece = jnp.dot(
                attended[:, h * cols : (h + 1) * cols], block, preferred_element_type=jnp.float32
            )
            total = piece if total is None else total + piece
        mixed = total.astype(jnp.bfloat16)
        for g in range(groups):
            o_ref[:, c, g] = mixed[g * count : (g + 1) * count].reshape(o_ref.shape[0], -1, cols)


def block(x, weights, groups):
    sources, total, rows, width = x.shape
    heads, seq, _, packed = weights.shape
    cols = packed // 4
    return pl.pallas_call(
        functools.partial(block_kernel, groups=groups),
        grid=(total // groups,),
        in_specs=[
            pl.BlockSpec((sources, groups, rows, width), lambda i: (0, i, 0, 0)),
            pl.BlockSpec(weights.shape, lambda i: (0, 0, 0, 0), pipeline_mode=pl.Buffered(1)),
        ],
        out_specs=pl.BlockSpec((sources, heads, groups, rows, cols), lambda i: (0, 0, i, 0, 0)),
        out_shape=jax.ShapeDtypeStruct((sources, heads, total, rows, cols), jnp.bfloat16),
        compiler_params=pltpu.CompilerParams(vmem_limit_bytes=56 * 1024 * 1024),
        cost_estimate=pl.CostEstimate(flops=10 * 2**30, transcendentals=2**21, bytes_accessed=12 * 2**20),
    )(x, weights)


def gather_weights(w_query, w_key, w_value, w_out, seq, head):
    s = lax.axis_index("seq")
    width, cols = w_query.shape
    rows = width // seq
    take = lambda w: lax.dynamic_slice_in_dim(w, s * rows, rows, 0)
    per_block = w_out.shape[0] // rows
    out = lax.dynamic_slice(w_out, ((s % per_block) * rows, (s // per_block) * cols), (rows, cols))
    mine = jnp.concatenate([take(w_query), take(w_key), take(w_value), out], axis=1)
    return lax.all_gather(mine, ("head", "seq"), axis=0, tiled=False).reshape(head, seq, rows, 4 * cols)


def local(seq, head, tokens, w_query, w_key, w_value, w_out):
    frames, patches, width = tokens.shape
    mine = patches // (seq * head)
    total = mine // GROUP
    rows = frames * GROUP
    weights = gather_weights(w_query, w_key, w_value, w_out, seq, head)
    h = lax.axis_index("head")
    x = tokens.reshape(frames, seq, head, mine, width)
    x = lax.dynamic_index_in_dim(x, h, axis=2, keepdims=False)
    x = x.reshape(frames, seq, total, GROUP, width)
    x = x.transpose(1, 2, 0, 3, 4).reshape(seq, total, rows, width)
    x = lax.all_to_all(x, "seq", split_axis=0, concat_axis=0, tiled=True)
    direct = rows % 16 == 0
    if not direct:
        x = x.transpose(1, 0, 2, 3).reshape(1, total, seq * rows, width)
    y = block(x, weights, 2)
    cols = y.shape[-1]
    if not direct:
        y = y.reshape(head, total, seq, rows, cols).transpose(2, 0, 1, 3, 4)
    y = y.reshape(seq * head, total * rows, cols)
    y = lax.all_to_all(y, ("seq", "head"), split_axis=0, concat_axis=0, tiled=True)
    y = y.reshape(seq * head, total, frames, GROUP, cols).transpose(2, 0, 1, 3, 4)
    return y.reshape(frames, patches, cols)


def solution(mesh):
    return jax.shard_map(
        functools.partial(local, mesh.shape["seq"], mesh.shape["head"]),
        mesh=mesh,
        in_specs=(
            P("seq", None, None),
            P(None, "head"),
            P(None, "head"),
            P(None, "head"),
            P("head", None),
        ),
        out_specs=P("seq", None, "head"),
        check_vma=False,
    )
```

```python
import functools

import jax
import jax.numpy as jnp
from jax import lax
from jax.experimental import pallas as pl
from jax.experimental.pallas import tpu as pltpu
from jax.sharding import PartitionSpec as P

HS = 64
GROUP = 4
LANES = 128

epsilon = 1e-05


def block_kernel(bits_ref, x_ref, *refs, groups, heads):
    piece_refs, o_ref, w_ref, sems = refs[:-3], refs[-3], refs[-2], refs[-1]
    width = x_ref.shape[-1]
    cols = o_ref.shape[-1]
    count = x_ref.shape[0] * x_ref.shape[2]
    slots = (bits_ref[0], 2 + bits_ref[1], 1 - bits_ref[0], 3 - bits_ref[1])

    def copies():
        made = []
        for h in range(heads):
            for half in range(2):
                pair, other_a, other_b = piece_refs[(h * 2 + half) * 3 : (h * 2 + half) * 3 + 3]
                sources = (pair.at[0], pair.at[1], other_a, other_b)
                for source, slot in zip(sources, slots):
                    made.append(
                        pltpu.make_async_copy(source, w_ref.at[h, half, slot], sems.at[len(made)])
                    )
        return made

    @pl.when(pl.program_id(0) == 0)
    def _():
        for copy in copies():
            copy.start()
        for copy in copies():
            copy.wait()

    x = jnp.concatenate([x_ref[:, g].reshape(count, width) for g in range(groups)], axis=0)
    values = x.astype(jnp.float32)
    centered = values - jnp.mean(values, axis=-1, keepdims=True)
    row_var = jnp.mean(centered * centered, axis=-1, keepdims=True)
    normed = (centered * lax.rsqrt(row_var + epsilon)).astype(jnp.bfloat16)
    row = lax.broadcasted_iota(jnp.int32, (2 * count, count), 0)
    col = lax.broadcasted_iota(jnp.int32, (2 * count, count), 1)
    same = (row % GROUP) == (col % GROUP)
    lane = lax.broadcasted_iota(jnp.int32, (count, LANES), 1)
    first = lane < HS
    attended = []
    for h in range(heads):
        weight = jnp.concatenate(
            [w_ref[h, half].reshape(width, 4 * LANES)[:, : 3 * LANES] for half in range(2)], axis=1
        )
        qkv = jnp.dot(normed, weight, preferred_element_type=jnp.float32).astype(jnp.bfloat16)
        for pair in range(2):
            at = pair * 3 * LANES
            parts = []
            for g in range(groups):
                span = slice(g * count, (g + 1) * count)
                q = qkv[span, at : at + LANES] * jnp.bfloat16(HS ** (-0.5))
                k = qkv[span, at + LANES : at + 2 * LANES]
                v = qkv[span, at + 2 * LANES : at + 3 * LANES]
                zero = jnp.zeros_like(q)
                both = jnp.concatenate([jnp.where(first, q, zero), jnp.where(first, zero, q)], axis=0)
                scores = lax.dot_general(
                    both, k, (((1,), (1,)), ((), ())), preferred_element_type=jnp.float32
                )
                scores = jnp.where(same, scores, -1e30)
                raised = jnp.exp(scores - jnp.max(scores, axis=1, keepdims=True))
                weights = (raised / jnp.sum(raised, axis=1, keepdims=True)).astype(jnp.bfloat16)
                out = jnp.dot(weights, v, preferred_element_type=jnp.float32)
                parts.append(jnp.where(first, out[:count], out[count:]).astype(jnp.bfloat16))
            attended.append(jnp.concatenate(parts, axis=0))
    attended = jnp.concatenate(attended, axis=1)
    for c in range(heads):
        total = None
        for h in range(heads):
            block = jnp.concatenate(
                [
                    jnp.concatenate(
                        [w_ref[h, half, c, i * LANES : (i + 1) * LANES, 3 * LANES :] for i in range(2)],
                        axis=1,
                    )
                    for half in range(2)
                ],
                axis=0,
            )
            piece = jnp.dot(
                attended[:, h * cols : (h + 1) * cols], block, preferred_element_type=jnp.float32
            )
            total = piece if total is None else total + piece
        mixed = total.astype(jnp.bfloat16)
        for g in range(groups):
            o_ref[:, c, g] = mixed[g * count : (g + 1) * count].reshape(o_ref.shape[0], -1, cols)


def block(bits, x, pieces, groups, heads, cols):
    sources, total, rows, width = x.shape
    return pl.pallas_call(
        functools.partial(block_kernel, groups=groups, heads=heads),
        grid=(total // groups,),
        in_specs=[
            pl.BlockSpec(memory_space=pltpu.SMEM),
            pl.BlockSpec((sources, groups, rows, width), lambda i: (0, i, 0, 0)),
        ]
        + [pl.BlockSpec(memory_space=pl.ANY)] * len(pieces),
        out_specs=pl.BlockSpec((sources, heads, groups, rows, cols), lambda i: (0, 0, i, 0, 0)),
        out_shape=jax.ShapeDtypeStruct((sources, heads, total, rows, cols), jnp.bfloat16),
        scratch_shapes=[
            pltpu.VMEM((heads, 2, 4, width // 4, 4 * LANES), jnp.bfloat16),
            pltpu.SemaphoreType.DMA((heads * 8,)),
        ],
        compiler_params=pltpu.CompilerParams(vmem_limit_bytes=56 * 1024 * 1024),
        cost_estimate=pl.CostEstimate(flops=10 * 2**30, transcendentals=2**21, bytes_accessed=12 * 2**20),
    )(bits, x, *pieces)


def gather_weights(w_query, w_key, w_value, w_out, seq, head):
    s = lax.axis_index("seq")
    low, mid, high = s & 1, (s >> 1) & 1, (s >> 2) & 1
    quarter = w_query.shape[0] // 4

    def piece(slot):
        take = lambda w: lax.dynamic_slice(w, (slot * quarter, low * LANES), (quarter, LANES))
        out = [
            lax.dynamic_slice(w_out, (low * LANES, slot * quarter + i * LANES), (LANES, LANES))
            for i in range(2)
        ]
        return jnp.concatenate(
            [take(w_query), take(w_key), take(w_value), jnp.concatenate(out, axis=0)], axis=1
        )

    flip = lambda v, bit: lax.ppermute(v, "seq", [(i, i ^ bit) for i in range(seq)])
    mine = jnp.stack([piece(mid), piece(2 + high)])
    moved = [mine] + [
        lax.ppermute(mine, "head", [(i, (i + k) % head) for i in range(head)]) for k in range(1, head)
    ]
    pieces = []
    for pair in moved:
        near = [pair, flip(pair[0], 2), flip(pair[1], 4)]
        pieces += near + [flip(v, 1) for v in near]
    return jnp.stack([mid, high]).astype(jnp.int32), pieces


def local(seq, head, tokens, w_query, w_key, w_value, w_out):
    frames, patches, width = tokens.shape
    mine = patches // (seq * head)
    total = mine // GROUP
    rows = frames * GROUP
    bits, pieces = gather_weights(w_query, w_key, w_value, w_out, seq, head)
    h = lax.axis_index("head")
    x = tokens.reshape(frames, seq, head, mine, width)
    x = lax.dynamic_index_in_dim(x, h, axis=2, keepdims=False)
    x = x.reshape(frames, seq, total, GROUP, width)
    x = x.transpose(1, 2, 0, 3, 4).reshape(seq, total, rows, width)
    x = lax.all_to_all(x, "seq", split_axis=0, concat_axis=0, tiled=True)
    direct = rows % 16 == 0
    if not direct:
        x = x.transpose(1, 0, 2, 3).reshape(1, total, seq * rows, width)
    cols = w_query.shape[1]
    y = block(bits, x, pieces, 2, head, cols)
    if not direct:
        y = y.reshape(head, total, seq, rows, cols).transpose(2, 0, 1, 3, 4)
    y = y.reshape(seq * head, total * rows, cols)
    y = lax.all_to_all(y, ("seq", "head"), split_axis=0, concat_axis=0, tiled=True)
    y = y.reshape(seq * head, total, frames, GROUP, cols).transpose(2, 0, 1, 3, 4)
    return y.reshape(frames, patches, cols)


def solution(mesh):
    return jax.shard_map(
        functools.partial(local, mesh.shape["seq"], mesh.shape["head"]),
        mesh=mesh,
        in_specs=(
            P("seq", None, None),
            P(None, "head"),
            P(None, "head"),
            P(None, "head"),
            P("head", None),
        ),
        out_specs=P("seq", None, "head"),
        check_vma=False,
    )
```

```python
import functools

import jax
import jax.numpy as jnp
from jax import lax
from jax.experimental import pallas as pl
from jax.experimental.pallas import tpu as pltpu
from jax.sharding import PartitionSpec as P

HS = 64
GROUP = 4
PARTS = 2
LANES = 128

epsilon = 1e-05


def block_kernel(bits_ref, x_ref, *refs, groups, heads):
    piece_refs, o_ref, w_ref, sems = refs[:-3], refs[-3], refs[-2], refs[-1]
    width = x_ref.shape[-1]
    cols = o_ref.shape[-1]
    count = x_ref.shape[0] * x_ref.shape[2]
    slots = (bits_ref[0], 2 + bits_ref[1], 1 - bits_ref[0], 3 - bits_ref[1])

    def copies():
        made = []
        for h in range(heads):
            for half in range(2):
                pair, other_a, other_b = piece_refs[(h * 2 + half) * 3 : (h * 2 + half) * 3 + 3]
                sources = (pair.at[0], pair.at[1], other_a, other_b)
                for source, slot in zip(sources, slots):
                    made.append(
                        pltpu.make_async_copy(source, w_ref.at[h, half, slot], sems.at[len(made)])
                    )
        return made

    @pl.when(pl.program_id(0) == 0)
    def _():
        for copy in copies():
            copy.start()
        for copy in copies():
            copy.wait()

    x = jnp.concatenate([x_ref[:, g].reshape(count, width) for g in range(groups)], axis=0)
    values = x.astype(jnp.float32)
    centered = values - jnp.mean(values, axis=-1, keepdims=True)
    row_var = jnp.mean(centered * centered, axis=-1, keepdims=True)
    normed = (centered * lax.rsqrt(row_var + epsilon)).astype(jnp.bfloat16)
    row = lax.broadcasted_iota(jnp.int32, (2 * count, count), 0)
    col = lax.broadcasted_iota(jnp.int32, (2 * count, count), 1)
    same = (row % GROUP) == (col % GROUP)
    lane = lax.broadcasted_iota(jnp.int32, (count, LANES), 1)
    first = lane < HS
    attended = []
    for h in range(heads):
        weight = jnp.concatenate(
            [w_ref[h, half].reshape(width, 4 * LANES)[:, : 3 * LANES] for half in range(2)], axis=1
        )
        qkv = jnp.dot(normed, weight, preferred_element_type=jnp.float32).astype(jnp.bfloat16)
        for pair in range(2):
            at = pair * 3 * LANES
            parts = []
            for g in range(groups):
                span = slice(g * count, (g + 1) * count)
                q = qkv[span, at : at + LANES] * jnp.bfloat16(HS ** (-0.5))
                k = qkv[span, at + LANES : at + 2 * LANES]
                v = qkv[span, at + 2 * LANES : at + 3 * LANES]
                zero = jnp.zeros_like(q)
                both = jnp.concatenate([jnp.where(first, q, zero), jnp.where(first, zero, q)], axis=0)
                scores = lax.dot_general(
                    both, k, (((1,), (1,)), ((), ())), preferred_element_type=jnp.float32
                )
                scores = jnp.where(same, scores, -1e30)
                raised = jnp.exp(scores - jnp.max(scores, axis=1, keepdims=True))
                weights = (raised / jnp.sum(raised, axis=1, keepdims=True)).astype(jnp.bfloat16)
                out = jnp.dot(weights, v, preferred_element_type=jnp.float32)
                parts.append(jnp.where(first, out[:count], out[count:]).astype(jnp.bfloat16))
            attended.append(jnp.concatenate(parts, axis=0))
    attended = jnp.concatenate(attended, axis=1)
    for c in range(heads):
        total = None
        for h in range(heads):
            block = jnp.concatenate(
                [
                    jnp.concatenate(
                        [w_ref[h, half, c, i * LANES : (i + 1) * LANES, 3 * LANES :] for i in range(2)],
                        axis=1,
                    )
                    for half in range(2)
                ],
                axis=0,
            )
            piece = jnp.dot(
                attended[:, h * cols : (h + 1) * cols], block, preferred_element_type=jnp.float32
            )
            total = piece if total is None else total + piece
        mixed = total.astype(jnp.bfloat16)
        for g in range(groups):
            o_ref[:, c, g] = mixed[g * count : (g + 1) * count].reshape(o_ref.shape[0], -1, cols)


def block(bits, x, pieces, groups, heads, cols, part, parts):
    sources, total, rows, width = x.shape
    total = total // parts
    offset = part * (total // groups)
    return pl.pallas_call(
        functools.partial(block_kernel, groups=groups, heads=heads),
        grid=(total // groups,),
        in_specs=[
            pl.BlockSpec(memory_space=pltpu.SMEM),
            pl.BlockSpec((sources, groups, rows, width), lambda i: (0, i + offset, 0, 0)),
        ]
        + [pl.BlockSpec(memory_space=pl.ANY)] * len(pieces),
        out_specs=pl.BlockSpec((sources, heads, groups, rows, cols), lambda i: (0, 0, i, 0, 0)),
        out_shape=jax.ShapeDtypeStruct((sources, heads, total, rows, cols), jnp.bfloat16),
        scratch_shapes=[
            pltpu.VMEM((heads, 2, 4, width // 4, 4 * LANES), jnp.bfloat16),
            pltpu.SemaphoreType.DMA((heads * 8,)),
        ],
        compiler_params=pltpu.CompilerParams(vmem_limit_bytes=56 * 1024 * 1024),
        cost_estimate=pl.CostEstimate(flops=10 * 2**30, transcendentals=2**21, bytes_accessed=12 * 2**20),
    )(bits, x, *pieces)


def gather_weights(w_query, w_key, w_value, w_out, seq, head):
    s = lax.axis_index("seq")
    low, mid, high = s & 1, (s >> 1) & 1, (s >> 2) & 1
    quarter = w_query.shape[0] // 4

    def piece(slot):
        take = lambda w: lax.dynamic_slice(w, (slot * quarter, low * LANES), (quarter, LANES))
        out = [
            lax.dynamic_slice(w_out, (low * LANES, slot * quarter + i * LANES), (LANES, LANES))
            for i in range(2)
        ]
        return jnp.concatenate(
            [take(w_query), take(w_key), take(w_value), jnp.concatenate(out, axis=0)], axis=1
        )

    flip = lambda v, bit: lax.ppermute(v, "seq", [(i, i ^ bit) for i in range(seq)])
    mine = jnp.stack([piece(mid), piece(2 + high)])
    moved = [mine] + [
        lax.ppermute(mine, "head", [(i, (i + k) % head) for i in range(head)]) for k in range(1, head)
    ]
    pieces = []
    for pair in moved:
        near = [pair, flip(pair[0], 2), flip(pair[1], 4)]
        pieces += near + [flip(v, 1) for v in near]
    return jnp.stack([mid, high]).astype(jnp.int32), pieces, mine


def local(seq, head, tokens, w_query, w_key, w_value, w_out):
    frames, patches, width = tokens.shape
    mine = patches // (seq * head)
    total = mine // GROUP
    rows = frames * GROUP
    bits, pieces, first = gather_weights(w_query, w_key, w_value, w_out, seq, head)
    h = lax.axis_index("head")
    tokens, h, _ = lax.optimization_barrier((tokens, h, first))
    x = tokens.reshape(frames, seq, head, mine, width)
    x = lax.dynamic_index_in_dim(x, h, axis=2, keepdims=False)
    x = x.reshape(frames, seq, total, GROUP, width)
    x = x.transpose(1, 2, 0, 3, 4).reshape(seq, total, rows, width)
    x = lax.all_to_all(x, "seq", split_axis=0, concat_axis=0, tiled=True)
    direct = rows % 16 == 0
    if not direct:
        x = x.transpose(1, 0, 2, 3).reshape(1, total, seq * rows, width)
    cols = w_query.shape[1]
    outs = []
    for part in range(PARTS):
        y = block(bits, x, pieces, 2, head, cols, part, PARTS)
        if not direct:
            y = y.reshape(head, total // PARTS, seq, rows, cols).transpose(2, 0, 1, 3, 4)
        y = y.reshape(seq * head, total // PARTS * rows, cols)
        y = lax.all_to_all(y, ("seq", "head"), split_axis=0, concat_axis=0, tiled=True)
        outs.append(y.reshape(seq * head, total // PARTS, frames, GROUP, cols).transpose(2, 0, 1, 3, 4))
    return jnp.concatenate(outs, axis=2).reshape(frames, patches, cols)


def solution(mesh):
    return jax.shard_map(
        functools.partial(local, mesh.shape["seq"], mesh.shape["head"]),
        mesh=mesh,
        in_specs=(
            P("seq", None, None),
            P(None, "head"),
            P(None, "head"),
            P(None, "head"),
            P("head", None),
        ),
        out_specs=P("seq", None, "head"),
        check_vma=False,
    )
```
